32 devices in a mesh: blk: 16 (over z, y, x), phe: 2 (over core).
Axes of the slice: x: 2, y: 2, z: 4, core: 2. Of those that a mesh axis runs over, the one named last changes fastest.
Arguments:
- ld_rows: bfloat16 [16384, 1024], P('blk'), may hold values from -1.5 to 1.5, as said below
- block_first: int32 [16384], P('blk'), may hold values from 0 to 16383, as said below
- beta_hat: float32 [128, 16384], P('phe', 'blk'), may hold values from -6 to 6
- psi: float32 [128, 16384], P('phe', 'blk'), may hold values from 0.05 to 5
- noise: bfloat16 [3, 128, 16384], P(None, 'phe', 'blk'), may hold values from -5 to 5
- sample_size: int32 [128], P('phe'), may hold values from 2000 to 199999
Outputs:
- effects: float32 [128, 16384], P('phe', 'blk')
The draws below stay inside these ranges and needn't reach their ends.
Inputs may be any that keep to these rules, and one draw needn't show every extreme that they name: block_first[j] is the first SNP of the run of consecutive SNPs that forms j's LD block; every block holds 128 to 1024 SNPs, except the last block, which ends at SNP 16384 - 1 and may hold fewer. ld_rows[j, c] is the LD between SNP j and SNP block_first[j] + c for c below the length of j's block, and zero for larger c; every block's matrix is symmetric with unit diagonal.
All inputs are finite; a program needn't handle non-finite values.
Results may differ from the reference program's by a relative error of at most 0.00055.
The reference program's roundings to bfloat16 on the way count: a program that leaves them out, or rounds other values in their place, can miss the bound.
Values may be sent and summed in bfloat16 or wider, within the bound.
No kernel may reach another device: no remote copies, remote signals or barrier semaphores. Data moves between devices by JAX's collectives and lax.ppermute only.
A program may use at most 64 MiB of HBM per device.

```python
import math
import jax
import jax.numpy as jnp
from jax import lax

BMAX = 1024
MINB = 128
ITERS = 3
NSNP = 16384
PHENO = 128


def block_layout(key):
    count = NSNP // MINB + 2
    lengths = jax.random.randint(jax.random.fold_in(key, 11), (count,), MINB, BMAX + 1).astype(jnp.int32)
    endings = jnp.cumsum(lengths).astype(jnp.int32)
    beginnings = endings - lengths
    positions = jnp.arange(NSNP, dtype=jnp.int32)
    member = jnp.searchsorted(endings, positions, side='right')
    first_snp = beginnings[member]
    block_size = jnp.minimum(endings[member], NSNP) - first_snp
    return (first_snp, block_size)


def draw_block_first(key, part):
    return block_layout(key)[0].astype(jnp.int32)


def draw_ld_rows(key, part):
    first_snp, block_size = block_layout(key)
    positions = jnp.arange(NSNP, dtype=jnp.int32)
    base_draw = jnp.clip(jax.random.normal(jax.random.fold_in(key, 12), (NSNP, BMAX), jnp.float32), -4.0, 4.0)
    offsets = jnp.arange(BMAX, dtype=jnp.int32)
    columns = first_snp[:, None] + offsets[None, :]
    inside = offsets[None, :] < block_size[:, None]
    mirror = base_draw[jnp.clip(columns, 0, NSNP - 1), (positions - first_snp)[:, None]]
    spread = 0.35 / math.sqrt(2.0) / jnp.sqrt(block_size.astype(jnp.float32))
    values = (base_draw + mirror) * spread[:, None]
    values = jnp.where(columns == positions[:, None], 1.0, values)
    values = jnp.where(inside, values, 0.0)
    return values.astype(jnp.bfloat16)


def touch_ends(entries, rng, least, high):
    index_at = [jax.random.randint(jax.random.fold_in(rng, axis), (), 0, length) for axis, length in enumerate(entries.shape)]
    longest = entries.shape.index(max(entries.shape))
    neighbour = index_at[:longest] + [(index_at[longest] + 1) % entries.shape[longest]] + index_at[longest + 1:]
    return entries.at[tuple(index_at)].set(least).at[tuple(neighbour)].set(high)


def block_levels(stream_key, shape, shards, smallest, top_value):
    def one(axis_at, blocks):
        heights = jax.random.uniform(jax.random.fold_in(jax.random.fold_in(stream_key, 6), axis_at), (blocks,), jnp.float32, smallest / len(shards), top_value / len(shards))
        return jnp.repeat(jnp.exp(heights), shape[axis_at] // blocks).reshape((-1,) + (1,) * (len(shape) - axis_at - 1))

    factor_of = one(*shards[0])
    for cut in shards[1:]:
        factor_of = factor_of * one(*cut)
    return factor_of


def gaussian(own_key, shape, deviation, limit, shards=(), held_as=jnp.bfloat16):
    values = deviation * jax.random.normal(own_key, shape, jnp.float32)
    if shards:
        values = values * block_levels(own_key, shape, shards, -0.22, 0.18)
    return jnp.clip(values, -limit, limit).astype(held_as)


def setup_inputs(seed: int = 0) -> dict:
    key_of = jax.random.split(jax.random.key(seed), 7)
    ld_rows = draw_ld_rows(jax.random.fold_in(key_of[6], 71), 0)
    block_first = draw_block_first(jax.random.fold_in(key_of[6], 71), 0)
    beta_hat = gaussian(key_of[2], (PHENO, NSNP), 1.0, 6.0, ((0, 2), (1, 16)), jnp.float32)
    psi = jnp.clip(jnp.exp(math.log(5.0) - 4.6051702 * jax.random.uniform(key_of[3], (PHENO, NSNP), jnp.float32) ** block_levels(key_of[3], (PHENO, NSNP), ((0, 2), (1, 16)), -0.2, 0.2)), 0.05, 5.0)
    noise = gaussian(key_of[4], (ITERS, PHENO, NSNP), 1.0, 5.0, ((1, 2), (2, 16)))
    sample_size = touch_ends(jax.random.randint(key_of[5], (PHENO,), 2000, 200000), jax.random.fold_in(key_of[5], 1), 2000, 199999).astype(jnp.int32)
    return dict(ld_rows=ld_rows, block_first=block_first, beta_hat=beta_hat, psi=psi, noise=noise, sample_size=sample_size)


tiny_term = 1e-06
sample_ref = 20000.0

def apply_blocks(rounded, ld_rows, block_first):
    positions = jnp.arange(NSNP, dtype=jnp.int32)
    starting = jnp.nonzero(block_first == positions, size=NSNP // MINB + 2, fill_value=NSNP)[0].astype(jnp.int32)
    block_count = jnp.sum((block_first == positions).astype(jnp.int32))
    following = jnp.concatenate([starting[1:], jnp.full((1,), NSNP, jnp.int32)])
    lengths = following - starting
    ld_padded = jnp.pad(ld_rows, ((0, BMAX), (0, 0)))
    low_padded = jnp.pad(rounded, ((0, 0), (0, BMAX)))
    offsets = jnp.arange(BMAX, dtype=jnp.int32)

    def one_block(number, result):
        row_start = starting[number]
        ld_tile = lax.dynamic_slice_in_dim(ld_padded, row_start, BMAX, 0)
        window = lax.dynamic_slice_in_dim(low_padded, row_start, BMAX, 1)
        product = lax.dot_general(window, ld_tile, (((1,), (1,)), ((), ())), preferred_element_type=jnp.float32)
        product = jnp.where((offsets < lengths[number])[None, :], product, jnp.float32(0.0))
        current = lax.dynamic_slice_in_dim(result, row_start, BMAX, 1)
        return lax.dynamic_update_slice_in_dim(result, current + product, row_start, 1)
    start_value = jnp.zeros((rounded.shape[0], NSNP + BMAX), jnp.float32)
    result = lax.fori_loop(0, block_count, one_block, start_value)
    return result[:, :NSNP]

def reference(ld_rows, block_first, beta_hat, psi, noise, sample_size):
    beta = jnp.zeros(beta_hat.shape, jnp.float32)
    for iteration in range(ITERS):
        rounded = beta.astype(jnp.bfloat16)
        grad = beta_hat - apply_blocks(rounded, ld_rows, block_first)
        resid = lax.optimization_barrier(jnp.sum(grad * grad, axis=1)) / NSNP + tiny_term
        weighted = beta * beta / psi
        scale = lax.optimization_barrier(jnp.sum(weighted, axis=1)) / NSNP + tiny_term
        pooled = jnp.sum(weighted) / (NSNP * PHENO) + tiny_term
        phi = (scale + pooled) / 2.0
        amp = jnp.sqrt(resid * sample_ref / sample_size.astype(jnp.float32))
        shrink = psi / (psi + phi[:, None])
        beta = shrink * (beta + grad + amp[:, None] * noise[iteration].astype(jnp.float32))
    return beta
```

```python
import functools

import jax
import jax.numpy as jnp
from jax import lax
from jax.experimental import pallas as pl
from jax.experimental.pallas import tpu as pltpu
from jax.sharding import PartitionSpec as P

ITERS = 3
LANES = 128
TILE = 256
WINDOWS = 3

tiny_term = 1e-06
sample_ref = 20000.0


def chunk_sums(values):
    total = values[:, :LANES]
    for at in range(LANES, values.shape[1], LANES):
        total = total + values[:, at : at + LANES]
    return total


def spread(resid, scale, out_ref):
    both = jnp.concatenate([chunk_sums(resid), chunk_sums(scale)], axis=0)
    row = jnp.sum(both.T, axis=0, keepdims=True)
    out_ref[...] = jnp.broadcast_to(row, out_ref.shape)


def first_sums(beta_hat_ref, out_ref):
    grad = beta_hat_ref[...]
    spread(grad * grad, jnp.zeros_like(grad), out_ref)


def update(own, groups, snps, sums_ref, sample_ref_, value_ref, psi_ref, noise_ref, beta_ref, low_ref=None):
    sums = sums_ref[...]
    half = sums.shape[1] // 2
    member = lax.rem(lax.broadcasted_iota(jnp.int32, sums.shape, 0), groups) == lax.axis_index(own)
    mine = jnp.sum(jnp.where(member, sums, 0.0), axis=0, keepdims=True)
    every = jnp.sum(sums, axis=0, keepdims=True)
    lane = lax.broadcasted_iota(jnp.int32, every.shape, 1)
    pooled = jnp.sum(jnp.where(lane >= half, every, 0.0), axis=1, keepdims=True)
    pooled = pooled / (snps * groups * half) + tiny_term
    mean = mine / snps + tiny_term
    amp = jnp.sqrt(mean * sample_ref / sample_ref_[...].astype(jnp.float32))
    phi = (mean + pooled) / 2.0
    table = jnp.broadcast_to(jnp.where(lane >= half, phi, amp), (2 * half, 2 * half)).T
    amp, phi = table[:half, :LANES], table[half:, :LANES]
    for at in range(0, psi_ref.shape[1], LANES):
        cut = slice(at, at + LANES)
        psi = psi_ref[:, cut]
        beta = psi / (psi + phi) * (value_ref[:, cut] + amp * noise_ref[0, :, cut].astype(jnp.float32))
        beta_ref[:, cut] = beta
        if low_ref is not None:
            low_ref[:, cut] = beta.astype(jnp.bfloat16)


def gradient(base_ref, firsts_ref, left_ref, low_ref, right_ref, ld_ref, beta_hat_ref, psi_ref, beta_ref, value_ref, out_ref, wide, windows):
    rows, span = ld_ref.shape
    phenos = low_ref.shape[0]
    base = base_ref[0]
    tiles = rows // TILE
    steps = firsts_ref.shape[0] // tiles
    for place, part in enumerate((left_ref, low_ref, right_ref)):
        wide[:, place * span : (place + 1) * span] = part[...]
    lane = lax.broadcasted_iota(jnp.int32, (phenos, LANES), 1)

    def fill(slot, first):
        start = first - base + span
        whole = pl.multiple_of(lax.div(start, LANES) * LANES, LANES)
        rest = start - whole
        turn = lax.rem(LANES - rest, LANES)
        keep = lane < LANES - rest
        now = pltpu.roll(wide[:, pl.ds(whole, LANES)].astype(jnp.float32), turn, 1)
        for at in range(0, span, LANES):
            after = pltpu.roll(wide[:, pl.ds(pl.multiple_of(whole + at + LANES, LANES), LANES)].astype(jnp.float32), turn, 1)
            windows[slot, :, at : at + LANES] = jnp.where(keep, now, after).astype(jnp.bfloat16)
            now = after

    slot = 0
    before = firsts_ref[0]
    fill(0, before)
    slots = []
    for number in range(tiles * steps):
        if number:
            first = firsts_ref[number]
            fresh = first != before
            slot = slot + fresh.astype(jnp.int32)

            @pl.when(fresh)
            def _(slot=slot, first=first):
                fill(slot, first)

            before = first
        slots.append((slot, before - base))

    resid = jnp.zeros((phenos, LANES), jnp.float32)
    scale = jnp.zeros((phenos, LANES), jnp.float32)
    for tile in range(tiles):
        cut = slice(tile * TILE, (tile + 1) * TILE)
        known = slots[tile * steps : (tile + 1) * steps]
        low = windows[pl.ds(known[0][0], WINDOWS)].reshape(WINDOWS * phenos, span)
        product = lax.dot_general(low, ld_ref[cut], (((1,), (1,)), ((), ())), preferred_element_type=jnp.float32)
        row = lax.broadcasted_iota(jnp.int32, (phenos, TILE), 1) + tile * TILE
        applied = product[:phenos]
        for turn in range(1, WINDOWS):
            begin = jnp.int32(rows)
            for other, where in reversed(known[1:]):
                begin = jnp.where(other == known[0][0] + turn, where, begin)
            applied = jnp.where(row >= begin, product[turn * phenos : (turn + 1) * phenos], applied)
        grad = beta_hat_ref[:, cut] - applied
        beta = beta_ref[:, cut]
        value_ref[:, cut] = beta + grad
        resid = resid + chunk_sums(grad * grad)
        scale = scale + chunk_sums(beta * beta / psi_ref[:, cut])
    spread(resid, scale, out_ref)


def shards(ld_rows, block_first, beta_hat, psi, noise, sample_size):
    rows, span = ld_rows.shape
    phenos = beta_hat.shape[0]
    blocks, groups = lax.axis_size("blk"), lax.axis_size("phe")
    snps = rows * blocks
    every = ("blk", "phe")
    base = jnp.reshape(lax.axis_index("blk") * rows, (1,)).astype(jnp.int32)
    ends = block_first.reshape(-1, LANES)
    firsts = jnp.stack([ends[:, 0], ends[:, LANES - 1]], axis=1).reshape(-1)
    samples = jnp.concatenate([sample_size, sample_size])[None]

    vmem = pl.BlockSpec(memory_space=pltpu.VMEM)
    smem = pl.BlockSpec(memory_space=pltpu.SMEM)
    sums_shape = jax.ShapeDtypeStruct((blocks * groups, 2 * phenos), jnp.float32)
    wide_shape = jax.ShapeDtypeStruct(beta_hat.shape, jnp.float32)
    low_shape = jax.ShapeDtypeStruct(beta_hat.shape, jnp.bfloat16)
    params = pltpu.CompilerParams(vmem_limit_bytes=16 << 20)

    def total(sums):
        return lax.all_to_all(sums, every, 0, 0, tiled=True)

    def step(t, sums, value):
        last = t == ITERS - 1
        return pl.pallas_call(
            functools.partial(update, "phe", groups, snps),
            grid=(1,),
            in_specs=[vmem] * 4 + [pl.BlockSpec((1,) + beta_hat.shape, lambda i: (t, 0, 0))],
            out_specs=vmem if last else [vmem] * 2,
            out_shape=wide_shape if last else [wide_shape, low_shape],
            compiler_params=params,
        )(sums, samples, value, psi, noise)

    sums = pl.pallas_call(
        first_sums, in_specs=[vmem], out_specs=vmem, out_shape=sums_shape, compiler_params=params
    )(beta_hat)
    value = beta_hat
    for t in range(ITERS - 1):
        beta, low = step(t, total(sums), value)
        left = lax.ppermute(low, "blk", [(i, i + 1) for i in range(blocks - 1)])
        right = lax.ppermute(low, "blk", [(i + 1, i) for i in range(blocks - 1)])
        value, sums = pl.pallas_call(
            gradient,
            in_specs=[smem] * 2 + [vmem] * 7,
            out_specs=[vmem] * 2,
            out_shape=[wide_shape, sums_shape],
            scratch_shapes=[
                pltpu.VMEM((phenos, 3 * span), jnp.bfloat16),
                pltpu.VMEM((2 * rows // LANES + WINDOWS, phenos, span), jnp.bfloat16),
            ],
            compiler_params=params,
        )(base, firsts, left, low, right, ld_rows, beta_hat, psi, beta)
    return step(ITERS - 1, total(sums), value)


def solution(mesh):
    in_specs = (
        P("blk", None),
        P("blk"),
        P("phe", "blk"),
        P("phe", "blk"),
        P(None, "phe", "blk"),
        P("phe"),
    )
    out_specs = P("phe", "blk")
    return jax.shard_map(shards, mesh=mesh, in_specs=in_specs, out_specs=out_specs, check_vma=False)
```

```python
import functools

import jax
import jax.numpy as jnp
from jax import lax
from jax.experimental import pallas as pl
from jax.experimental.pallas import tpu as pltpu
from jax.sharding import PartitionSpec as P


ITERS = 3
LANES = 128
TILE = 256
WINDOWS = 3

tiny_term = 1e-06
sample_ref = 20000.0


def chunk_sums(values):
    total = values[:, :LANES]
    for at in range(LANES, values.shape[1], LANES):
        total = total + values[:, at : at + LANES]
    return total


def spread(resid, scale, out_ref):
    both = jnp.concatenate([chunk_sums(resid), chunk_sums(scale)], axis=0)
    row = jnp.sum(both.T, axis=0, keepdims=True)
    out_ref[...] = jnp.broadcast_to(row, out_ref.shape)


def first_sums(beta_hat_ref, kept_ref, out_ref, sem):
    copy = pltpu.make_async_copy(beta_hat_ref, kept_ref, sem)
    copy.start()
    copy.wait()
    grad = kept_ref[...]
    spread(grad * grad, jnp.zeros_like(grad), out_ref)


def load(block_first_ref, psi_ref, noise_ref, ld_ref, psi_out, noise_out, ld_out, table_ref, starts, sems):
    pairs = (block_first_ref, starts), (psi_ref, psi_out), (noise_ref, noise_out), (ld_ref, ld_out)
    copies = [pltpu.make_async_copy(a, b, sems.at[n]) for n, (a, b) in enumerate(pairs)]
    for copy in copies:
        copy.start()
    copies[0].wait()
    first = starts[...]
    row = lax.broadcasted_iota(jnp.int32, first.shape, 0) * 2
    lane = lax.broadcasted_iota(jnp.int32, first.shape, 1)
    start = jnp.where(lane == row, jnp.broadcast_to(first[:, :1], first.shape), 0)
    end = jnp.where(lane == row + 1, jnp.broadcast_to(first[:, LANES - 1 :], first.shape), 0)
    table_ref[...] = jnp.sum(start + end, axis=0, keepdims=True)
    for copy in copies[1:]:
        copy.wait()


def update(own, groups, snps, sums_ref, sample_size_ref, value_ref, psi_ref, noise_ref, beta_ref, low_ref=None):
    sums = sums_ref[...]
    half = sums.shape[1] // 2
    member = lax.rem(lax.broadcasted_iota(jnp.int32, sums.shape, 0), groups) == lax.axis_index(own)
    mine = jnp.sum(jnp.where(member, sums, 0.0), axis=0, keepdims=True)
    every = jnp.sum(sums, axis=0, keepdims=True)
    lane = lax.broadcasted_iota(jnp.int32, every.shape, 1)
    pooled = jnp.sum(jnp.where(lane >= half, every, 0.0), axis=1, keepdims=True)
    pooled = pooled / (snps * groups * half) + tiny_term
    mean = mine / snps + tiny_term
    samples = sample_size_ref[...].astype(jnp.float32)
    amp = jnp.sqrt(mean * sample_ref / jnp.concatenate([samples, samples], axis=1))
    phi = (mean + pooled) / 2.0
    table = jnp.broadcast_to(jnp.where(lane >= half, phi, amp), (2 * half, 2 * half)).T
    amp, phi = table[:half, :LANES], table[half:, :LANES]
    for at in range(0, psi_ref.shape[1], LANES):
        cut = slice(at, at + LANES)
        psi = psi_ref[:, cut]
        beta = psi / (psi + phi) * (value_ref[:, cut] + amp * noise_ref[0, :, cut].astype(jnp.float32))
        beta_ref[:, cut] = beta
        if low_ref is not None:
            low_ref[:, cut] = beta.astype(jnp.bfloat16)


def gradient(along, firsts_ref, far_ref, low_ref, near_ref, ld_ref, beta_hat_ref, psi_ref, beta_ref, value_ref, out_ref, wide, windows):
    rows, span = ld_ref.shape
    phenos = low_ref.shape[0]
    place = lax.axis_index(along)
    base = place * rows
    odd = lax.rem(place, 2)
    tiles = rows // TILE
    steps = 2 * TILE // LANES
    for third, part in ((0, far_ref), (1, low_ref), (2, near_ref)):
        at = pl.multiple_of(jnp.where(odd == 1, 2 - third, third) * span, LANES)
        wide[:, pl.ds(at, span)] = part[...]
    lane = lax.broadcasted_iota(jnp.int32, (phenos, LANES), 1)

    def fill(slot, first):
        start = first - base + span
        whole = pl.multiple_of(lax.div(start, LANES) * LANES, LANES)
        rest = start - whole
        turn = lax.rem(LANES - rest, LANES)
        keep = lane < LANES - rest
        now = pltpu.roll(wide[:, pl.ds(whole, LANES)].astype(jnp.float32), turn, 1)
        for at in range(0, span, LANES):
            after = pltpu.roll(wide[:, pl.ds(pl.multiple_of(whole + at + LANES, LANES), LANES)].astype(jnp.float32), turn, 1)
            windows[slot, :, at : at + LANES] = jnp.where(keep, now, after).astype(jnp.bfloat16)
            now = after

    slot = 0
    before = firsts_ref[0, 0]
    fill(0, before)
    slots = []
    for number in range(tiles * steps):
        if number:
            first = firsts_ref[0, number]
            fresh = first != before
            slot = slot + fresh.astype(jnp.int32)

            @pl.when(fresh)
            def _(slot=slot, first=first):
                fill(slot, first)

            before = first
        slots.append((slot, before - base))

    resid = jnp.zeros((phenos, LANES), jnp.float32)
    scale = jnp.zeros((phenos, LANES), jnp.float32)
    for tile in range(tiles):
        cut = slice(tile * TILE, (tile + 1) * TILE)
        known = slots[tile * steps : (tile + 1) * steps]
        low = windows[pl.ds(known[0][0], WINDOWS)].reshape(WINDOWS * phenos, span)
        product = lax.dot_general(low, ld_ref[cut], (((1,), (1,)), ((), ())), preferred_element_type=jnp.float32)
        row = lax.broadcasted_iota(jnp.int32, (phenos, TILE), 1) + tile * TILE
        applied = product[:phenos]
        for turn in range(1, WINDOWS):
            begin = jnp.int32(rows)
            for other, where in reversed(known[1:]):
                begin = jnp.where(other == known[0][0] + turn, where, begin)
            applied = jnp.where(row >= begin, product[turn * phenos : (turn + 1) * phenos], applied)
        grad = beta_hat_ref[:, cut] - applied
        beta = beta_ref[:, cut]
        value_ref[:, cut] = beta + grad
        resid = resid + chunk_sums(grad * grad)
        scale = scale + chunk_sums(beta * beta / psi_ref[:, cut])
    spread(resid, scale, out_ref)


def shards(ld_rows, block_first, beta_hat, psi, noise, sample_size):
    rows, span = ld_rows.shape
    phenos = beta_hat.shape[0]
    blocks, groups = lax.axis_size("blk"), lax.axis_size("phe")
    snps = rows * blocks
    every = ("blk", "phe")
    vmem = pl.BlockSpec(memory_space=pltpu.VMEM)
    smem = pl.BlockSpec(memory_space=pltpu.SMEM)
    hbm = pl.BlockSpec(memory_space=pltpu.HBM)
    wide_shape = pltpu.VMEM(beta_hat.shape, jnp.float32)
    low_shape = pltpu.VMEM(beta_hat.shape, jnp.bfloat16)
    sums_shape = pltpu.VMEM((blocks * groups, 2 * phenos), jnp.float32)
    params = pltpu.CompilerParams(vmem_limit_bytes=16 << 20)

    def here(argument):
        return pltpu.with_memory_space_constraint(argument, pltpu.HBM)

    def total(sums):
        return lax.all_to_all(sums, every, 0, 0, tiled=True)

    beta_hat, sums = pl.pallas_call(
        first_sums,
        in_specs=[hbm],
        out_specs=[vmem] * 2,
        out_shape=[wide_shape, sums_shape],
        scratch_shapes=[pltpu.SemaphoreType.DMA],
        compiler_params=params,
    )(here(beta_hat))
    sums = total(sums)
    psi, noise, ld_rows, firsts = pl.pallas_call(
        load,
        in_specs=[hbm] * 4,
        out_specs=[vmem] * 4,
        out_shape=[wide_shape, pltpu.VMEM(noise.shape, noise.dtype), pltpu.VMEM(ld_rows.shape, ld_rows.dtype), pltpu.VMEM((1, LANES), jnp.int32)],
        scratch_shapes=[pltpu.VMEM((rows // LANES, LANES), jnp.int32), pltpu.SemaphoreType.DMA((4,))],
        compiler_params=params,
        cost_estimate=pl.CostEstimate(flops=1 << 24, bytes_accessed=3 << 20, transcendentals=0),
    )(*map(here, (block_first.reshape(-1, LANES), psi, noise, ld_rows)))

    def step(t, sums, value):
        last = t == ITERS - 1
        return pl.pallas_call(
            functools.partial(update, "phe", groups, snps),
            grid=(1,),
            in_specs=[vmem] * 4 + [pl.BlockSpec((1,) + beta_hat.shape, lambda i: (t, 0, 0))],
            out_specs=vmem if last else [vmem] * 2,
            out_shape=jax.ShapeDtypeStruct(beta_hat.shape, jnp.float32) if last else [wide_shape, low_shape],
            compiler_params=params,
        )(sums, sample_size[None], value, psi, noise)

    far = [(i, i + 1 if i % 2 else i - 1) for i in range(1, blocks - 1 + blocks % 2)]
    near = [(i, i ^ 1) for i in range(blocks - blocks % 2)]
    value = beta_hat
    for t in range(ITERS - 1):
        beta, low = step(t, sums, value)
        far_low = lax.ppermute(low, "blk", far)
        near_low = lax.ppermute(low, "blk", near)
        value, sums = pl.pallas_call(
            functools.partial(gradient, "blk"),
            in_specs=[smem] + [vmem] * 7,
            out_specs=[vmem] * 2,
            out_shape=[wide_shape, sums_shape],
            scratch_shapes=[
                pltpu.VMEM((phenos, 3 * span), jnp.bfloat16),
                pltpu.VMEM((2 * rows // LANES + WINDOWS, phenos, span), jnp.bfloat16),
            ],
            compiler_params=params,
        )(firsts, far_low, low, near_low, ld_rows, beta_hat, psi, beta)
        sums = total(sums)
    return step(ITERS - 1, sums, value)


def solution(mesh):
    in_specs = (
        P("blk", None),
        P("blk"),
        P("phe", "blk"),
        P("phe", "blk"),
        P(None, "phe", "blk"),
        P("phe"),
    )
    out_specs = P("phe", "blk")
    return jax.shard_map(shards, mesh=mesh, in_specs=in_specs, out_specs=out_specs, check_vma=False)
```

```python
import functools

import jax
import jax.numpy as jnp
from jax import lax
from jax.experimental import pallas as pl
from jax.experimental.pallas import tpu as pltpu
from jax.sharding import PartitionSpec as P


ITERS = 3
LANES = 128
TILE = 256
WINDOWS = 3

tiny_term = 1e-06
sample_ref = 20000.0


def chunk_sums(values):
    total = values[:, :LANES]
    for at in range(LANES, values.shape[1], LANES):
        total = total + values[:, at : at + LANES]
    return total


def spread(resid, scale, out_ref):
    both = jnp.concatenate([chunk_sums(resid), chunk_sums(scale)], axis=0)
    row = jnp.sum(both.T, axis=0, keepdims=True)
    out_ref[...] = jnp.broadcast_to(row, out_ref.shape)


def first_sums(beta_hat_ref, kept_ref, out_ref, sem):
    copy = pltpu.make_async_copy(beta_hat_ref, kept_ref, sem)
    copy.start()
    copy.wait()
    grad = kept_ref[...]
    spread(grad * grad, jnp.zeros_like(grad), out_ref)


def load(block_first_ref, psi_ref, noise_ref, ld_ref, psi_out, noise_out, ld_out, table_ref, starts, sems):
    pairs = (block_first_ref, starts), (psi_ref, psi_out), (noise_ref, noise_out), (ld_ref, ld_out)
    copies = [pltpu.make_async_copy(a, b, sems.at[n]) for n, (a, b) in enumerate(pairs)]
    for copy in copies:
        copy.start()
    copies[0].wait()
    first = starts[...]
    row = lax.broadcasted_iota(jnp.int32, first.shape, 0) * 2
    lane = lax.broadcasted_iota(jnp.int32, first.shape, 1)
    start = jnp.where(lane == row, jnp.broadcast_to(first[:, :1], first.shape), 0)
    end = jnp.where(lane == row + 1, jnp.broadcast_to(first[:, LANES - 1 :], first.shape), 0)
    table_ref[...] = jnp.sum(start + end, axis=0, keepdims=True)
    for copy in copies[1:]:
        copy.wait()


def update(own, groups, snps, sums_ref, sample_size_ref, value_ref, psi_ref, noise_ref, beta_ref, low_ref=None):
    sums = sums_ref[...]
    half = sums.shape[1] // 2
    member = lax.rem(lax.broadcasted_iota(jnp.int32, sums.shape, 0), groups) == lax.axis_index(own)
    mine = jnp.sum(jnp.where(member, sums, 0.0), axis=0, keepdims=True)
    every = jnp.sum(sums, axis=0, keepdims=True)
    lane = lax.broadcasted_iota(jnp.int32, every.shape, 1)
    pooled = jnp.sum(jnp.where(lane >= half, every, 0.0), axis=1, keepdims=True)
    pooled = pooled / (snps * groups * half) + tiny_term
    mean = mine / snps + tiny_term
    samples = sample_size_ref[...].astype(jnp.float32)
    amp = jnp.sqrt(mean * sample_ref / jnp.concatenate([samples, samples], axis=1))
    phi = (mean + pooled) / 2.0
    table = jnp.broadcast_to(jnp.where(lane >= half, phi, amp), (2 * half, 2 * half)).T
    amp, phi = table[:half, :LANES], table[half:, :LANES]
    for at in range(0, psi_ref.shape[1], LANES):
        cut = slice(at, at + LANES)
        psi = psi_ref[:, cut]
        beta = psi / (psi + phi) * (value_ref[:, cut] + amp * noise_ref[0, :, cut].astype(jnp.float32))
        beta_ref[:, cut] = beta
        if low_ref is not None:
            low_ref[:, cut] = beta.astype(jnp.bfloat16)


def turned(buffer, start, store):
    phenos = buffer.shape[0]
    whole = pl.multiple_of(lax.div(start, LANES) * LANES, LANES)
    rest = start - whole
    turn = lax.rem(LANES - rest, LANES)
    keep = lax.broadcasted_iota(jnp.int32, (phenos, LANES), 1) < LANES - rest

    def piece(at):
        return pltpu.roll(buffer[:, pl.ds(pl.multiple_of(whole + at, LANES), LANES)].astype(jnp.float32), turn, 1)

    now = piece(0)
    for at in range(0, (buffer.shape[1] - LANES) // 3 // LANES * LANES, LANES):
        after = piece(at + LANES)
        store(slice(at, at + LANES), jnp.where(keep, now, after).astype(jnp.bfloat16))
        now = after


def product_with(low, ld_ref, cut):
    return lax.dot_general(low, ld_ref[cut], (((1,), (1,)), ((), ())), preferred_element_type=jnp.float32)


def inner(along, firsts_ref, low_ref, ld_ref, beta_hat_ref, psi_ref, beta_ref, grad_ref, scale_ref, wide, windows, slots):
    rows, span = ld_ref.shape
    phenos = low_ref.shape[0]
    base = lax.axis_index(along) * rows
    tiles = rows // TILE
    steps = 2 * TILE // LANES
    wide[...] = jnp.zeros_like(wide)
    wide[:, span : 2 * span] = low_ref[...]

    def fill(slot, first):
        def store(cut, values):
            windows[slot, :, cut] = values

        turned(wide, first - base + span, store)

    fill(0, firsts_ref[0, 0])
    slots[0] = 0

    def look(number, slot):
        first = firsts_ref[0, number]
        fresh = first != firsts_ref[0, number - 1]
        slot = slot + fresh.astype(jnp.int32)
        slots[number] = slot

        @pl.when(fresh)
        def _():
            fill(slot, first)

        return slot

    lax.fori_loop(1, tiles * steps, look, jnp.int32(0))
    scale = jnp.zeros((phenos, LANES), jnp.float32)
    for tile in range(tiles):
        cut = slice(tile * TILE, (tile + 1) * TILE)
        known = [(slots[number], firsts_ref[0, number] - base) for number in range(tile * steps, (tile + 1) * steps)]
        product = product_with(windows[pl.ds(known[0][0], WINDOWS)].reshape(WINDOWS * phenos, span), ld_ref, cut)
        row = lax.broadcasted_iota(jnp.int32, (phenos, TILE), 1) + tile * TILE
        applied = product[:phenos]
        for turn in range(1, WINDOWS):
            begin = jnp.int32(rows)
            for other, where in reversed(known[1:]):
                begin = jnp.where(other == known[0][0] + turn, where, begin)
            applied = jnp.where(row >= begin, product[turn * phenos : (turn + 1) * phenos], applied)
        grad_ref[:, cut] = beta_hat_ref[:, cut] - applied
        beta = beta_ref[:, cut]
        scale = scale + chunk_sums(beta * beta / psi_ref[:, cut])
    scale_ref[...] = scale


def outer(along, firsts_ref, far_ref, near_ref, ld_ref, grad_ref, scale_ref, beta_ref, value_ref, out_ref, sides, windows):
    rows, span = ld_ref.shape
    phenos = far_ref.shape[0]
    place = lax.axis_index(along)
    base = place * rows
    odd = lax.rem(place, 2) == 1
    gap = span + LANES
    sides[:, span : span + gap] = jnp.zeros((phenos, gap), sides.dtype)
    sides[:, pl.ds(pl.multiple_of(jnp.where(odd, span + gap, 0), LANES), span)] = far_ref[...]
    sides[:, pl.ds(pl.multiple_of(jnp.where(odd, 0, span + gap), LANES), span)] = near_ref[...]
    table = firsts_ref[...]
    count = 2 * rows // LANES
    first = table[0, 0] - base
    last = table[0, count - 1] - base
    lane = lax.broadcasted_iota(jnp.int32, table.shape, 1)
    ends = jnp.where((lane < count) & (table - base != first), table - base, rows)
    end = jnp.min(ends.astype(jnp.float32), axis=1, keepdims=True).astype(jnp.int32)

    def store_at(begin):
        def store(cut, values):
            windows[begin : begin + phenos, cut] = values

        return store

    turned(sides, first + span, store_at(0))
    turned(sides, jnp.maximum(last, 0) + gap, store_at(phenos))
    resid = jnp.zeros((phenos, LANES), jnp.float32)
    for tile in range(rows // TILE):
        cut = slice(tile * TILE, (tile + 1) * TILE)
        product = product_with(windows[...], ld_ref, cut)
        row = lax.broadcasted_iota(jnp.int32, (phenos, TILE), 1) + tile * TILE
        applied = jnp.where(row < end, product[:phenos], 0.0) + jnp.where(row >= last, product[phenos:], 0.0)
        grad = grad_ref[:, cut] - applied
        value_ref[:, cut] = beta_ref[:, cut] + grad
        resid = resid + chunk_sums(grad * grad)
    spread(resid, scale_ref[...], out_ref)


def shards(ld_rows, block_first, beta_hat, psi, noise, sample_size):
    rows, span = ld_rows.shape
    phenos = beta_hat.shape[0]
    blocks, groups = lax.axis_size("blk"), lax.axis_size("phe")
    snps = rows * blocks
    every = ("blk", "phe")
    vmem = pl.BlockSpec(memory_space=pltpu.VMEM)
    smem = pl.BlockSpec(memory_space=pltpu.SMEM)
    hbm = pl.BlockSpec(memory_space=pltpu.HBM)
    wide_shape = pltpu.VMEM(beta_hat.shape, jnp.float32)
    low_shape = pltpu.VMEM(beta_hat.shape, jnp.bfloat16)
    sums_shape = pltpu.VMEM((blocks * groups, 2 * phenos), jnp.float32)
    params = pltpu.CompilerParams(vmem_limit_bytes=16 << 20)

    def here(argument):
        return pltpu.with_memory_space_constraint(argument, pltpu.HBM)

    def total(sums):
        return lax.all_to_all(sums, every, 0, 0, tiled=True)

    beta_hat, sums = pl.pallas_call(
        first_sums,
        in_specs=[hbm],
        out_specs=[vmem] * 2,
        out_shape=[wide_shape, sums_shape],
        scratch_shapes=[pltpu.SemaphoreType.DMA],
        compiler_params=params,
    )(here(beta_hat))
    sums = total(sums)
    psi, noise, ld_rows, firsts = pl.pallas_call(
        load,
        in_specs=[hbm] * 4,
        out_specs=[vmem] * 4,
        out_shape=[wide_shape, pltpu.VMEM(noise.shape, noise.dtype), pltpu.VMEM(ld_rows.shape, ld_rows.dtype), pltpu.VMEM((1, LANES), jnp.int32)],
        scratch_shapes=[pltpu.VMEM((rows // LANES, LANES), jnp.int32), pltpu.SemaphoreType.DMA((4,))],
        compiler_params=params,
        cost_estimate=pl.CostEstimate(flops=1 << 24, bytes_accessed=3 << 20, transcendentals=0),
    )(*map(here, (block_first.reshape(-1, LANES), psi, noise, ld_rows)))

    def step(t, sums, value):
        last = t == ITERS - 1
        return pl.pallas_call(
            functools.partial(update, "phe", groups, snps),
            grid=(1,),
            in_specs=[vmem] * 4 + [pl.BlockSpec((1,) + beta_hat.shape, lambda i: (t, 0, 0))],
            out_specs=vmem if last else [vmem] * 2,
            out_shape=jax.ShapeDtypeStruct(beta_hat.shape, jnp.float32) if last else [wide_shape, low_shape],
            compiler_params=params,
        )(sums, sample_size[None], value, psi, noise)

    far = [(i, i + 1 if i % 2 else i - 1) for i in range(1, blocks - 1 + blocks % 2)]
    near = [(i, i ^ 1) for i in range(blocks - blocks % 2)]
    value = beta_hat
    for t in range(ITERS - 1):
        beta, low = step(t, sums, value)
        far_low = lax.ppermute(low, "blk", far)
        near_low = lax.ppermute(low, "blk", near)
        grad, scale = pl.pallas_call(
            functools.partial(inner, "blk"),
            in_specs=[smem] + [vmem] * 5,
            out_specs=[vmem] * 2,
            out_shape=[wide_shape, pltpu.VMEM((phenos, LANES), jnp.float32)],
            scratch_shapes=[
                pltpu.VMEM((phenos, 3 * span + LANES), jnp.bfloat16),
                pltpu.VMEM((2 * rows // LANES + WINDOWS, phenos, span), jnp.bfloat16),
                pltpu.SMEM((2 * rows // LANES,), jnp.int32),
            ],
            compiler_params=params,
            cost_estimate=pl.CostEstimate(flops=2 * WINDOWS * phenos * rows * span, bytes_accessed=4 << 20, transcendentals=0),
        )(firsts, low, ld_rows, beta_hat, psi, beta)
        value, sums = pl.pallas_call(
            functools.partial(outer, "blk"),
            in_specs=[vmem] * 7,
            out_specs=[vmem] * 2,
            out_shape=[wide_shape, sums_shape],
            scratch_shapes=[
                pltpu.VMEM((phenos, 3 * span + LANES), jnp.bfloat16),
                pltpu.VMEM((2 * phenos, span), jnp.bfloat16),
            ],
            compiler_params=params,
        )(firsts, far_low, near_low, ld_rows, grad, scale, beta)
        sums = total(sums)
    return step(ITERS - 1, sums, value)


def solution(mesh):
    in_specs = (
        P("blk", None),
        P("blk"),
        P("phe", "blk"),
        P("phe", "blk"),
        P(None, "phe", "blk"),
        P("phe"),
    )
    out_specs = P("phe", "blk")
    return jax.shard_map(shards, mesh=mesh, in_specs=in_specs, out_specs=out_specs, check_vma=False)
```

```python
import functools

import jax
import jax.numpy as jnp
from jax import lax
from jax.experimental import pallas as pl
from jax.experimental.pallas import tpu as pltpu
from jax.sharding import PartitionSpec as P


ITERS = 3
LANES = 128
TILE = 256
WINDOWS = 3

tiny_term = 1e-06
sample_ref = 20000.0


def chunk_sums(values):
    total = values[:, :LANES]
    for at in range(LANES, values.shape[1], LANES):
        total = total + values[:, at : at + LANES]
    return total


def spread(resid, scale, out_ref):
    both = jnp.concatenate([chunk_sums(resid), chunk_sums(scale)], axis=0)
    row = jnp.sum(both.T, axis=0, keepdims=True)
    out_ref[...] = jnp.broadcast_to(row, out_ref.shape)


def begin(beta_hat_ref, psi_ref, noise_ref, size_ref, beta_hat_out, psi_out, noise_out, size_out, out_ref, sems):
    pairs = (beta_hat_ref, beta_hat_out), (psi_ref, psi_out), (noise_ref, noise_out), (size_ref, size_out)
    copies = [pltpu.make_async_copy(a, b, sems.at[n]) for n, (a, b) in enumerate(pairs)]
    for copy in copies:
        copy.start()
    copies[0].wait()
    grad = beta_hat_out[...]
    spread(grad * grad, jnp.zeros_like(grad), out_ref)
    for copy in copies[1:]:
        copy.wait()


def load(after_ref, block_first_ref, ld_ref, ld_out, table_ref, starts, sems):
    pairs = (block_first_ref, starts), (ld_ref, ld_out)
    copies = [pltpu.make_async_copy(a, b, sems.at[n]) for n, (a, b) in enumerate(pairs)]
    for copy in copies:
        copy.start()
    copies[0].wait()
    first = starts[...]
    row = lax.broadcasted_iota(jnp.int32, first.shape, 0) * 2
    lane = lax.broadcasted_iota(jnp.int32, first.shape, 1)
    start = jnp.where(lane == row, jnp.broadcast_to(first[:, :1], first.shape), 0)
    end = jnp.where(lane == row + 1, jnp.broadcast_to(first[:, LANES - 1 :], first.shape), 0)
    table_ref[...] = jnp.sum(start + end, axis=0, keepdims=True)
    copies[1].wait()


def update(own, groups, snps, t, sums_ref, sample_size_ref, value_ref, psi_ref, noise_ref, beta_ref, low_ref=None):
    sums = sums_ref[...]
    half = sums.shape[1] // 2
    member = lax.rem(lax.broadcasted_iota(jnp.int32, sums.shape, 0), groups) == lax.axis_index(own)
    mine = jnp.sum(jnp.where(member, sums, 0.0), axis=0, keepdims=True)
    every = jnp.sum(sums, axis=0, keepdims=True)
    lane = lax.broadcasted_iota(jnp.int32, every.shape, 1)
    pooled = jnp.sum(jnp.where(lane >= half, every, 0.0), axis=1, keepdims=True)
    pooled = pooled / (snps * groups * half) + tiny_term
    mean = mine / snps + tiny_term
    samples = sample_size_ref[...].astype(jnp.float32)
    amp = jnp.sqrt(mean * sample_ref / jnp.concatenate([samples, samples], axis=1))
    phi = (mean + pooled) / 2.0
    table = jnp.broadcast_to(jnp.where(lane >= half, phi, amp), (2 * half, 2 * half)).T
    amp, phi = table[:half, :LANES], table[half:, :LANES]
    for at in range(0, psi_ref.shape[1], LANES):
        cut = slice(at, at + LANES)
        psi = psi_ref[:, cut]
        beta = psi / (psi + phi) * (value_ref[:, cut] + amp * noise_ref[t, :, cut].astype(jnp.float32))
        beta_ref[:, cut] = beta
        if low_ref is not None:
            low_ref[:, cut] = beta.astype(jnp.bfloat16)


def turned(buffer, start, store):
    phenos = buffer.shape[0]
    whole = pl.multiple_of(lax.div(start, LANES) * LANES, LANES)
    rest = start - whole
    turn = lax.rem(LANES - rest, LANES)
    keep = lax.broadcasted_iota(jnp.int32, (phenos, LANES), 1) < LANES - rest

    def piece(at):
        return pltpu.roll(buffer[:, pl.ds(pl.multiple_of(whole + at, LANES), LANES)].astype(jnp.float32), turn, 1)

    now = piece(0)
    for at in range(0, (buffer.shape[1] - LANES) // 3 // LANES * LANES, LANES):
        after = piece(at + LANES)
        store(slice(at, at + LANES), jnp.where(keep, now, after).astype(jnp.bfloat16))
        now = after


def product_with(low, ld_ref, cut):
    return lax.dot_general(low, ld_ref[cut], (((1,), (1,)), ((), ())), preferred_element_type=jnp.float32)


def inner(along, firsts_ref, low_ref, ld_ref, beta_hat_ref, psi_ref, beta_ref, grad_ref, scale_ref, wide, windows, slots):
    rows, span = ld_ref.shape
    phenos = low_ref.shape[0]
    base = lax.axis_index(along) * rows
    tiles = rows // TILE
    steps = 2 * TILE // LANES
    wide[...] = jnp.zeros_like(wide)
    wide[:, span : 2 * span] = low_ref[...]

    def fill(slot, first):
        def store(cut, values):
            windows[slot, :, cut] = values

        turned(wide, first - base + span, store)

    fill(0, firsts_ref[0, 0])
    slots[0] = 0

    def look(number, slot):
        first = firsts_ref[0, number]
        fresh = first != firsts_ref[0, number - 1]
        slot = slot + fresh.astype(jnp.int32)
        slots[number] = slot

        @pl.when(fresh)
        def _():
            fill(slot, first)

        return slot

    lax.fori_loop(1, tiles * steps, look, jnp.int32(0))
    scale = jnp.zeros((phenos, LANES), jnp.float32)
    for tile in range(tiles):
        cut = slice(tile * TILE, (tile + 1) * TILE)
        known = [(slots[number], firsts_ref[0, number] - base) for number in range(tile * steps, (tile + 1) * steps)]
        product = product_with(windows[pl.ds(known[0][0], WINDOWS)].reshape(WINDOWS * phenos, span), ld_ref, cut)
        row = lax.broadcasted_iota(jnp.int32, (phenos, TILE), 1) + tile * TILE
        applied = product[:phenos]
        for turn in range(1, WINDOWS):
            begin = jnp.int32(rows)
            for other, where in reversed(known[1:]):
                begin = jnp.where(other == known[0][0] + turn, where, begin)
            applied = jnp.where(row >= begin, product[turn * phenos : (turn + 1) * phenos], applied)
        grad_ref[:, cut] = beta_hat_ref[:, cut] - applied
        beta = beta_ref[:, cut]
        scale = scale + chunk_sums(beta * beta / psi_ref[:, cut])
    scale_ref[...] = scale


def outer(along, firsts_ref, far_ref, near_ref, ld_ref, grad_ref, scale_ref, beta_ref, value_ref, out_ref, sides, windows):
    rows, span = ld_ref.shape
    phenos = far_ref.shape[0]
    place = lax.axis_index(along)
    base = place * rows
    odd = lax.rem(place, 2) == 1
    gap = span + LANES
    sides[:, span : span + gap] = jnp.zeros((phenos, gap), sides.dtype)
    sides[:, pl.ds(pl.multiple_of(jnp.where(odd, span + gap, 0), LANES), span)] = far_ref[...]
    sides[:, pl.ds(pl.multiple_of(jnp.where(odd, 0, span + gap), LANES), span)] = near_ref[...]
    table = firsts_ref[...]
    count = 2 * rows // LANES
    first = table[0, 0] - base
    last = table[0, count - 1] - base
    lane = lax.broadcasted_iota(jnp.int32, table.shape, 1)
    ends = jnp.where((lane < count) & (table - base != first), table - base, rows)
    end = jnp.min(ends.astype(jnp.float32), axis=1, keepdims=True).astype(jnp.int32)

    def store_at(begin):
        def store(cut, values):
            windows[begin : begin + phenos, cut] = values

        return store

    turned(sides, first + span, store_at(0))
    turned(sides, jnp.maximum(last, 0) + gap, store_at(phenos))
    resid = jnp.zeros((phenos, LANES), jnp.float32)
    for tile in range(rows // TILE):
        cut = slice(tile * TILE, (tile + 1) * TILE)
        product = product_with(windows[...], ld_ref, cut)
        row = lax.broadcasted_iota(jnp.int32, (phenos, TILE), 1) + tile * TILE
        applied = jnp.where(row < end, product[:phenos], 0.0) + jnp.where(row >= last, product[phenos:], 0.0)
        grad = grad_ref[:, cut] - applied
        value_ref[:, cut] = beta_ref[:, cut] + grad
        resid = resid + chunk_sums(grad * grad)
    spread(resid, scale_ref[...], out_ref)


def shards(ld_rows, block_first, beta_hat, psi, noise, sample_size):
    rows, span = ld_rows.shape
    phenos = beta_hat.shape[0]
    blocks, groups = lax.axis_size("blk"), lax.axis_size("phe")
    snps = rows * blocks
    every = ("blk", "phe")
    vmem = pl.BlockSpec(memory_space=pltpu.VMEM)
    smem = pl.BlockSpec(memory_space=pltpu.SMEM)
    hbm = pl.BlockSpec(memory_space=pltpu.HBM)
    wide_shape = pltpu.VMEM(beta_hat.shape, jnp.float32)
    low_shape = pltpu.VMEM(beta_hat.shape, jnp.bfloat16)
    sums_shape = pltpu.VMEM((blocks * groups, 2 * phenos), jnp.float32)
    params = pltpu.CompilerParams(vmem_limit_bytes=16 << 20)

    def here(argument):
        return pltpu.with_memory_space_constraint(argument, pltpu.HBM)

    def total(sums):
        return lax.all_to_all(sums, every, 0, 0, tiled=True)

    beta_hat, psi, noise, sample_size, sums = pl.pallas_call(
        begin,
        in_specs=[hbm] * 4,
        out_specs=[vmem] * 5,
        out_shape=[
            wide_shape,
            wide_shape,
            pltpu.VMEM(noise.shape, noise.dtype),
            pltpu.VMEM((1, phenos), jnp.int32),
            sums_shape,
        ],
        scratch_shapes=[pltpu.SemaphoreType.DMA((4,))],
        compiler_params=params,
    )(*map(here, (beta_hat, psi, noise, sample_size[None])))
    sums = total(sums)

    def step(t, sums, value):
        last = t == ITERS - 1
        return pl.pallas_call(
            functools.partial(update, "phe", groups, snps, t),
            in_specs=[vmem] * 5,
            out_specs=vmem if last else [vmem] * 2,
            out_shape=jax.ShapeDtypeStruct(beta_hat.shape, jnp.float32) if last else [wide_shape, low_shape],
            compiler_params=params,
        )(sums, sample_size, value, psi, noise)

    far = [(i, i + 1 if i % 2 else i - 1) for i in range(1, blocks - 1 + blocks % 2)]
    near = [(i, i ^ 1) for i in range(blocks - blocks % 2)]
    value = beta_hat
    for t in range(ITERS - 1):
        beta, low = step(t, sums, value)
        far_low = lax.ppermute(low, "blk", far)
        near_low = lax.ppermute(low, "blk", near)
        if t == 0:
            ld_rows, firsts = pl.pallas_call(
                load,
                in_specs=[vmem] + [hbm] * 2,
                out_specs=[vmem] * 2,
                out_shape=[pltpu.VMEM(ld_rows.shape, ld_rows.dtype), pltpu.VMEM((1, LANES), jnp.int32)],
                scratch_shapes=[pltpu.VMEM((rows // LANES, LANES), jnp.int32), pltpu.SemaphoreType.DMA((2,))],
                compiler_params=params,
                cost_estimate=pl.CostEstimate(flops=1 << 26, bytes_accessed=3 << 20, transcendentals=0),
            )(low, here(block_first.reshape(-1, LANES)), here(ld_rows))
        grad, scale = pl.pallas_call(
            functools.partial(inner, "blk"),
            in_specs=[smem] + [vmem] * 5,
            out_specs=[vmem] * 2,
            out_shape=[wide_shape, pltpu.VMEM((phenos, LANES), jnp.float32)],
            scratch_shapes=[
                pltpu.VMEM((phenos, 3 * span + LANES), jnp.bfloat16),
                pltpu.VMEM((2 * rows // LANES + WINDOWS, phenos, span), jnp.bfloat16),
                pltpu.SMEM((2 * rows // LANES,), jnp.int32),
            ],
            compiler_params=params,
            cost_estimate=pl.CostEstimate(flops=2 * WINDOWS * phenos * rows * span, bytes_accessed=4 << 20, transcendentals=0),
        )(firsts, low, ld_rows, beta_hat, psi, beta)
        value, sums = pl.pallas_call(
            functools.partial(outer, "blk"),
            in_specs=[vmem] * 7,
            out_specs=[vmem] * 2,
            out_shape=[wide_shape, sums_shape],
            scratch_shapes=[
                pltpu.VMEM((phenos, 3 * span + LANES), jnp.bfloat16),
                pltpu.VMEM((2 * phenos, span), jnp.bfloat16),
            ],
            compiler_params=params,
        )(firsts, far_low, near_low, ld_rows, grad, scale, beta)
        sums = total(sums)
    return step(ITERS - 1, sums, value)


def solution(mesh):
    in_specs = (
        P("blk", None),
        P("blk"),
        P("phe", "blk"),
        P("phe", "blk"),
        P(None, "phe", "blk"),
        P("phe"),
    )
    out_specs = P("phe", "blk")
    return jax.shard_map(shards, mesh=mesh, in_specs=in_specs, out_specs=out_specs, check_vma=False)
```

```python
import functools

import jax
import jax.numpy as jnp
from jax import lax
from jax.experimental import pallas as pl
from jax.experimental.pallas import tpu as pltpu
from jax.sharding import PartitionSpec as P


ITERS = 3
LANES = 128
TILE = 256
WINDOWS = 3

tiny_term = 1e-06
sample_ref = 20000.0


def chunk_sums(values):
    total = values[:, :LANES]
    for at in range(LANES, values.shape[1], LANES):
        total = total + values[:, at : at + LANES]
    return total


def spread(resid, scale, out_ref):
    both = jnp.concatenate([chunk_sums(resid), chunk_sums(scale)], axis=0)
    row = jnp.sum(both.T, axis=0, keepdims=True)
    out_ref[...] = jnp.broadcast_to(row, out_ref.shape)


def begin(beta_hat_ref, psi_ref, noise_ref, size_ref, beta_hat_out, psi_out, noise_out, size_out, out_ref, sems):
    pairs = (beta_hat_ref, beta_hat_out), (psi_ref, psi_out), (noise_ref, noise_out), (size_ref, size_out)
    copies = [pltpu.make_async_copy(a, b, sems.at[n]) for n, (a, b) in enumerate(pairs)]
    for copy in copies:
        copy.start()
    copies[0].wait()
    grad = beta_hat_out[...]
    spread(grad * grad, jnp.zeros_like(grad), out_ref)
    for copy in copies[1:]:
        copy.wait()


def load(after_ref, block_first_ref, ld_ref, ld_out, table_ref, starts, sems):
    pairs = (block_first_ref, starts), (ld_ref, ld_out)
    copies = [pltpu.make_async_copy(a, b, sems.at[n]) for n, (a, b) in enumerate(pairs)]
    for copy in copies:
        copy.start()
    copies[0].wait()
    first = starts[...]
    row = lax.broadcasted_iota(jnp.int32, first.shape, 0) * 2
    lane = lax.broadcasted_iota(jnp.int32, first.shape, 1)
    start = jnp.where(lane == row, jnp.broadcast_to(first[:, :1], first.shape), 0)
    end = jnp.where(lane == row + 1, jnp.broadcast_to(first[:, LANES - 1 :], first.shape), 0)
    table_ref[...] = jnp.sum(start + end, axis=0, keepdims=True)
    copies[1].wait()


def update(own, groups, snps, t, sums_ref, sample_size_ref, value_ref, psi_ref, noise_ref, beta_ref, low_ref=None):
    sums = sums_ref[...]
    half = sums.shape[1] // 2
    member = lax.rem(lax.broadcasted_iota(jnp.int32, sums.shape, 0), groups) == lax.axis_index(own)
    mine = jnp.sum(jnp.where(member, sums, 0.0), axis=0, keepdims=True)
    every = jnp.sum(sums, axis=0, keepdims=True)
    lane = lax.broadcasted_iota(jnp.int32, every.shape, 1)
    pooled = jnp.sum(jnp.where(lane >= half, every, 0.0), axis=1, keepdims=True)
    pooled = pooled / (snps * groups * half) + tiny_term
    mean = mine / snps + tiny_term
    samples = sample_size_ref[...].astype(jnp.float32)
    amp = jnp.sqrt(mean * sample_ref / jnp.concatenate([samples, samples], axis=1))
    phi = (mean + pooled) / 2.0
    table = jnp.broadcast_to(jnp.where(lane >= half, phi, amp), (2 * half, 2 * half)).T
    amp, phi = table[:half, :LANES], table[half:, :LANES]
    for at in range(0, psi_ref.shape[1], LANES):
        cut = slice(at, at + LANES)
        psi = psi_ref[:, cut]
        beta = psi / (psi + phi) * (value_ref[:, cut] + amp * noise_ref[t, :, cut].astype(jnp.float32))
        beta_ref[:, cut] = beta
        if low_ref is not None:
            low_ref[:, cut] = beta.astype(jnp.bfloat16)


def turned(buffer, start, width, store):
    phenos = buffer.shape[0]
    whole = pl.multiple_of(lax.div(start, LANES) * LANES, LANES)
    rest = start - whole
    turn = lax.rem(LANES - rest, LANES)
    keep = lax.broadcasted_iota(jnp.int32, (phenos, LANES), 1) < LANES - rest

    def piece(at):
        return pltpu.roll(buffer[:, pl.ds(pl.multiple_of(whole + at, LANES), LANES)].astype(jnp.float32), turn, 1)

    now = piece(0)
    for at in range(0, width, LANES):
        after = piece(at + LANES)
        store(slice(at, at + LANES), jnp.where(keep, now, after).astype(jnp.bfloat16))
        now = after


def product_with(low, ld):
    return lax.dot_general(low, ld, (((1,), (1,)), ((), ())), preferred_element_type=jnp.float32)


def inner(along, firsts_ref, low_ref, ld_ref, beta_hat_ref, psi_ref, beta_ref, grad_ref, scale_ref, wide, windows, slots):
    rows, span = ld_ref.shape
    phenos = low_ref.shape[0]
    base = lax.axis_index(along) * rows
    tiles = rows // TILE
    steps = 2 * TILE // LANES
    wide[...] = jnp.zeros_like(wide)
    wide[:, span : 2 * span] = low_ref[...]

    def fill(slot, first):
        def store(cut, values):
            windows[slot, :, cut] = values

        turned(wide, first - base + span, span, store)

    fill(0, firsts_ref[0, 0])
    slots[0] = 0

    def look(number, slot):
        first = firsts_ref[0, number]
        fresh = first != firsts_ref[0, number - 1]
        slot = slot + fresh.astype(jnp.int32)
        slots[number] = slot

        @pl.when(fresh)
        def _():
            fill(slot, first)

        return slot

    lax.fori_loop(1, tiles * steps, look, jnp.int32(0))
    scale = jnp.zeros((phenos, LANES), jnp.float32)
    for tile in range(tiles):
        cut = slice(tile * TILE, (tile + 1) * TILE)
        known = [(slots[number], firsts_ref[0, number] - base) for number in range(tile * steps, (tile + 1) * steps)]
        product = product_with(windows[pl.ds(known[0][0], WINDOWS)].reshape(WINDOWS * phenos, span), ld_ref[cut])
        row = lax.broadcasted_iota(jnp.int32, (phenos, TILE), 1) + tile * TILE
        applied = product[:phenos]
        for turn in range(1, WINDOWS):
            begin = jnp.int32(rows)
            for other, where in reversed(known[1:]):
                begin = jnp.where(other == known[0][0] + turn, where, begin)
            applied = jnp.where(row >= begin, product[turn * phenos : (turn + 1) * phenos], applied)
        grad_ref[:, cut] = beta_hat_ref[:, cut] - applied
        beta = beta_ref[:, cut]
        scale = scale + chunk_sums(beta * beta / psi_ref[:, cut])
    scale_ref[...] = scale


def outer(along, far, firsts_ref, halo_ref, ld_ref, grad_ref, *refs):
    rows, span = ld_ref.shape
    phenos = halo_ref.shape[0]
    sides, window = refs[-2:]
    place = lax.axis_index(along)
    base = place * rows
    left = lax.rem(place, 2) == (0 if far else 1)
    gap = span + LANES
    sides[:, :gap] = jnp.zeros((phenos, gap), sides.dtype)
    sides[:, gap : gap + span] = halo_ref[...]
    sides[:, gap + span :] = jnp.zeros((phenos, gap), sides.dtype)
    table = firsts_ref[...]
    count = 2 * rows // LANES
    first = table[0, 0] - base
    last = table[0, count - 1] - base
    lane = lax.broadcasted_iota(jnp.int32, table.shape, 1)
    ends = jnp.where((lane < count) & (table - base != first), table - base, rows)
    end = jnp.min(ends.astype(jnp.float32), axis=1, keepdims=True).astype(jnp.int32)
    low_row = jnp.where(left, 0, last)
    high_row = jnp.where(left, end, rows)

    def store(cut, values):
        window[:, cut] = values

    turned(sides, jnp.where(left, first + span + gap, jnp.maximum(last, 0) + LANES), span, store)
    resid = jnp.zeros((phenos, LANES), jnp.float32)
    tiles = rows // TILE
    for turn in range(tiles):
        width = span - turn * TILE
        begin = pl.multiple_of(jnp.where(left, turn, tiles - 1 - turn) * TILE, TILE)
        cut, part = pl.ds(begin, TILE), pl.ds(pl.multiple_of(jnp.where(left, 0, span - width), TILE), width)
        row = lax.broadcasted_iota(jnp.int32, (phenos, TILE), 1) + begin
        inside = (row >= low_row) & (row < high_row)
        grad = grad_ref[:, cut] - jnp.where(inside, product_with(window[:, part], ld_ref[cut, part]), 0.0)
        if not far:
            refs[0][:, cut] = grad
            continue
        refs[2][:, cut] = refs[1][:, cut] + grad
        resid = resid + chunk_sums(grad * grad)
    if far:
        spread(resid, refs[0][...], refs[3])


def shards(ld_rows, block_first, beta_hat, psi, noise, sample_size):
    rows, span = ld_rows.shape
    phenos = beta_hat.shape[0]
    blocks, groups = lax.axis_size("blk"), lax.axis_size("phe")
    assert rows == span and rows % TILE == 0, rows
    snps = rows * blocks
    every = ("blk", "phe")
    vmem = pl.BlockSpec(memory_space=pltpu.VMEM)
    smem = pl.BlockSpec(memory_space=pltpu.SMEM)
    hbm = pl.BlockSpec(memory_space=pltpu.HBM)
    wide_shape = pltpu.VMEM(beta_hat.shape, jnp.float32)
    low_shape = pltpu.VMEM(beta_hat.shape, jnp.bfloat16)
    sums_shape = pltpu.VMEM((blocks * groups, 2 * phenos), jnp.float32)
    params = pltpu.CompilerParams(vmem_limit_bytes=16 << 20)

    def here(argument):
        return pltpu.with_memory_space_constraint(argument, pltpu.HBM)

    def total(sums):
        return lax.all_to_all(sums, every, 0, 0, tiled=True)

    beta_hat, psi, noise, sample_size, sums = pl.pallas_call(
        begin,
        in_specs=[hbm] * 4,
        out_specs=[vmem] * 5,
        out_shape=[
            wide_shape,
            wide_shape,
            pltpu.VMEM(noise.shape, noise.dtype),
            pltpu.VMEM((1, phenos), jnp.int32),
            sums_shape,
        ],
        scratch_shapes=[pltpu.SemaphoreType.DMA((4,))],
        compiler_params=params,
    )(*map(here, (beta_hat, psi, noise, sample_size[None])))
    sums = total(sums)

    def step(t, sums, value):
        last = t == ITERS - 1
        return pl.pallas_call(
            functools.partial(update, "phe", groups, snps, t),
            in_specs=[vmem] * 5,
            out_specs=vmem if last else [vmem] * 2,
            out_shape=jax.ShapeDtypeStruct(beta_hat.shape, jnp.float32) if last else [wide_shape, low_shape],
            compiler_params=params,
        )(sums, sample_size, value, psi, noise)

    far = [(i, i + 1 if i % 2 else i - 1) for i in range(1, blocks - 1 + blocks % 2)]
    near = [(i, i ^ 1) for i in range(blocks - blocks % 2)]
    value = beta_hat
    for t in range(ITERS - 1):
        beta, low = step(t, sums, value)
        far_low = lax.ppermute(low, "blk", far)
        near_low = lax.ppermute(low, "blk", near)
        if t == 0:
            ld_rows, firsts = pl.pallas_call(
                load,
                in_specs=[vmem] + [hbm] * 2,
                out_specs=[vmem] * 2,
                out_shape=[pltpu.VMEM(ld_rows.shape, ld_rows.dtype), pltpu.VMEM((1, LANES), jnp.int32)],
                scratch_shapes=[pltpu.VMEM((rows // LANES, LANES), jnp.int32), pltpu.SemaphoreType.DMA((2,))],
                compiler_params=params,
                cost_estimate=pl.CostEstimate(flops=1 << 26, bytes_accessed=3 << 20, transcendentals=0),
            )(low, here(block_first.reshape(-1, LANES)), here(ld_rows))
        grad, scale = pl.pallas_call(
            functools.partial(inner, "blk"),
            in_specs=[smem] + [vmem] * 5,
            out_specs=[vmem] * 2,
            out_shape=[wide_shape, pltpu.VMEM((phenos, LANES), jnp.float32)],
            scratch_shapes=[
                pltpu.VMEM((phenos, 3 * span + LANES), jnp.bfloat16),
                pltpu.VMEM((2 * rows // LANES + WINDOWS, phenos, span), jnp.bfloat16),
                pltpu.SMEM((2 * rows // LANES,), jnp.int32),
            ],
            compiler_params=params,
            cost_estimate=pl.CostEstimate(flops=2 * WINDOWS * phenos * rows * span, bytes_accessed=4 << 20, transcendentals=0),
        )(firsts, low, ld_rows, beta_hat, psi, beta)
        sides = [pltpu.VMEM((phenos, 3 * span + 2 * LANES), jnp.bfloat16), pltpu.VMEM((phenos, span), jnp.bfloat16)]
        grad = pl.pallas_call(
            functools.partial(outer, "blk", False),
            in_specs=[vmem] * 4,
            out_specs=vmem,
            out_shape=wide_shape,
            scratch_shapes=sides,
            compiler_params=params,
            cost_estimate=pl.CostEstimate(flops=2 * phenos * rows * span, bytes_accessed=3 << 20, transcendentals=0),
        )(firsts, near_low, ld_rows, grad)
        value, sums = pl.pallas_call(
            functools.partial(outer, "blk", True),
            in_specs=[vmem] * 6,
            out_specs=[vmem] * 2,
            out_shape=[wide_shape, sums_shape],
            scratch_shapes=sides,
            compiler_params=params,
        )(firsts, far_low, ld_rows, grad, scale, beta)
        sums = total(sums)
    return step(ITERS - 1, sums, value)


def solution(mesh):
    in_specs = (
        P("blk", None),
        P("blk"),
        P("phe", "blk"),
        P("phe", "blk"),
        P(None, "phe", "blk"),
        P("phe"),
    )
    out_specs = P("phe", "blk")
    return jax.shard_map(shards, mesh=mesh, in_specs=in_specs, out_specs=out_specs, check_vma=False)
```

```python
import functools

import jax
import jax.numpy as jnp
from jax import lax
from jax.experimental import pallas as pl
from jax.experimental.pallas import tpu as pltpu
from jax.sharding import PartitionSpec as P


ITERS = 3
LANES = 128
TILE = 256
WINDOWS = 3

tiny_term = 1e-06
sample_ref = 20000.0


def chunk_sums(values):
    total = values[:, :LANES]
    for at in range(LANES, values.shape[1], LANES):
        total = total + values[:, at : at + LANES]
    return total


def spread(resid, scale, out_ref):
    both = jnp.concatenate([chunk_sums(resid), chunk_sums(scale)], axis=0)
    row = jnp.sum(both.T, axis=0, keepdims=True)
    out_ref[...] = jnp.broadcast_to(row, out_ref.shape)


def begin(beta_hat_ref, psi_ref, noise_ref, size_ref, beta_hat_out, psi_out, noise_out, size_out, out_ref, sems):
    pairs = (beta_hat_ref, beta_hat_out), (psi_ref, psi_out), (noise_ref, noise_out), (size_ref, size_out)
    copies = [pltpu.make_async_copy(a, b, sems.at[n]) for n, (a, b) in enumerate(pairs)]
    for copy in copies:
        copy.start()
    copies[0].wait()
    grad = beta_hat_out[...]
    spread(grad * grad, jnp.zeros_like(grad), out_ref)
    for copy in copies[1:]:
        copy.wait()


def load(after_ref, block_first_ref, ld_ref, ld_out, table_ref, starts, sems):
    pairs = (block_first_ref, starts), (ld_ref, ld_out)
    copies = [pltpu.make_async_copy(a, b, sems.at[n]) for n, (a, b) in enumerate(pairs)]
    for copy in copies:
        copy.start()
    copies[0].wait()
    first = starts[...]
    row = lax.broadcasted_iota(jnp.int32, first.shape, 0) * 2
    lane = lax.broadcasted_iota(jnp.int32, first.shape, 1)
    start = jnp.where(lane == row, jnp.broadcast_to(first[:, :1], first.shape), 0)
    end = jnp.where(lane == row + 1, jnp.broadcast_to(first[:, LANES - 1 :], first.shape), 0)
    table_ref[...] = jnp.sum(start + end, axis=0, keepdims=True)
    copies[1].wait()


def update(own, groups, snps, t, sums_ref, sample_size_ref, value_ref, psi_ref, noise_ref, beta_ref, low_ref=None):
    sums = sums_ref[...]
    half = sums.shape[1] // 2
    member = lax.rem(lax.broadcasted_iota(jnp.int32, sums.shape, 0), groups) == lax.axis_index(own)
    mine = jnp.sum(jnp.where(member, sums, 0.0), axis=0, keepdims=True)
    every = jnp.sum(sums, axis=0, keepdims=True)
    lane = lax.broadcasted_iota(jnp.int32, every.shape, 1)
    pooled = jnp.sum(jnp.where(lane >= half, every, 0.0), axis=1, keepdims=True)
    pooled = pooled / (snps * groups * half) + tiny_term
    mean = mine / snps + tiny_term
    samples = sample_size_ref[...].astype(jnp.float32)
    amp = jnp.sqrt(mean * sample_ref / jnp.concatenate([samples, samples], axis=1))
    phi = (mean + pooled) / 2.0
    table = jnp.broadcast_to(jnp.where(lane >= half, phi, amp), (2 * half, 2 * half)).T
    amp, phi = table[:half, :LANES], table[half:, :LANES]
    for at in range(0, psi_ref.shape[1], LANES):
        cut = slice(at, at + LANES)
        psi = psi_ref[:, cut]
        beta = psi / (psi + phi) * (value_ref[:, cut] + amp * noise_ref[t, :, cut].astype(jnp.float32))
        beta_ref[:, cut] = beta
        if low_ref is not None:
            low_ref[:, cut] = beta.astype(jnp.bfloat16)


def turned(buffer, start, width, store, inside=None):
    phenos = buffer.shape[0]
    whole = pl.multiple_of(lax.div(start, LANES) * LANES, LANES)
    rest = start - whole
    turn = lax.rem(LANES - rest, LANES)
    keep = lax.broadcasted_iota(jnp.int32, (phenos, LANES), 1) < LANES - rest

    def piece(at):
        return pltpu.roll(buffer[:, pl.ds(pl.multiple_of(whole + at, LANES), LANES)].astype(jnp.float32), turn, 1)

    now = piece(0)
    for at in range(0, width, LANES):
        after = piece(at + LANES)
        values = jnp.where(keep, now, after)
        values = values if inside is None else jnp.where(inside, values, 0.0)
        store(slice(at, at + LANES), values.astype(jnp.bfloat16))
        now = after


def product_with(low, ld):
    return lax.dot_general(low, ld, (((1,), (1,)), ((), ())), preferred_element_type=jnp.float32)


def inner(along, firsts_ref, low_ref, ld_ref, beta_hat_ref, psi_ref, beta_ref, grad_ref, scale_ref, wide, windows, slots):
    rows, span = ld_ref.shape
    phenos = low_ref.shape[0]
    base = lax.axis_index(along) * rows
    tiles = rows // TILE
    steps = 2 * TILE // LANES
    wide[...] = jnp.zeros_like(wide)
    wide[:, span : 2 * span] = low_ref[...]

    def fill(slot, first):
        def store(cut, values):
            windows[slot, :, cut] = values

        turned(wide, first - base + span, span, store)

    fill(0, firsts_ref[0, 0])
    slots[0] = 0

    def look(number, slot):
        first = firsts_ref[0, number]
        fresh = first != firsts_ref[0, number - 1]
        slot = slot + fresh.astype(jnp.int32)
        slots[number] = slot

        @pl.when(fresh)
        def _():
            fill(slot, first)

        return slot

    lax.fori_loop(1, tiles * steps, look, jnp.int32(0))
    scale = jnp.zeros((phenos, LANES), jnp.float32)
    for tile in range(tiles):
        cut = slice(tile * TILE, (tile + 1) * TILE)
        known = [(slots[number], firsts_ref[0, number] - base) for number in range(tile * steps, (tile + 1) * steps)]
        product = product_with(windows[pl.ds(known[0][0], WINDOWS)].reshape(WINDOWS * phenos, span), ld_ref[cut])
        row = lax.broadcasted_iota(jnp.int32, (phenos, TILE), 1) + tile * TILE
        applied = product[:phenos]
        for turn in range(1, WINDOWS):
            begin = jnp.int32(rows)
            for other, where in reversed(known[1:]):
                begin = jnp.where(other == known[0][0] + turn, where, begin)
            applied = jnp.where(row >= begin, product[turn * phenos : (turn + 1) * phenos], applied)
        grad_ref[:, cut] = beta_hat_ref[:, cut] - applied
        beta = beta_ref[:, cut]
        scale = scale + chunk_sums(beta * beta / psi_ref[:, cut])
    scale_ref[...] = scale


def outer(along, far, firsts_ref, halo_ref, ld_ref, grad_ref, *refs):
    rows, span = ld_ref.shape
    phenos = halo_ref.shape[0]
    sides, window = refs[-2:]
    place = lax.axis_index(along)
    base = place * rows
    left = lax.rem(place, 2) == (0 if far else 1)
    gap = span + LANES
    sides[:, :gap] = jnp.zeros((phenos, gap), sides.dtype)
    sides[:, gap : gap + span] = halo_ref[...]
    sides[:, gap + span :] = jnp.zeros((phenos, gap), sides.dtype)
    table = firsts_ref[...]
    count = 2 * rows // LANES
    first = table[0, 0] - base
    last = table[0, count - 1] - base
    lane = lax.broadcasted_iota(jnp.int32, table.shape, 1)
    ends = jnp.where((lane < count) & (table - base != first), table - base, rows)
    end = jnp.min(ends.astype(jnp.float32), axis=1, keepdims=True).astype(jnp.int32)
    low_row = jnp.where(left, 0, last)
    high_row = jnp.where(left, end, rows)

    def store(cut, values):
        window[:, cut] = values

    turned(sides, jnp.where(left, first + span + gap, jnp.maximum(last, 0) + LANES), span, store)
    resid = jnp.zeros((phenos, LANES), jnp.float32)
    tiles = rows // TILE
    for turn in range(tiles):
        width = span - turn * TILE
        begin = pl.multiple_of(jnp.where(left, turn, tiles - 1 - turn) * TILE, TILE)
        cut, part = pl.ds(begin, TILE), pl.ds(pl.multiple_of(jnp.where(left, 0, span - width), TILE), width)
        row = lax.broadcasted_iota(jnp.int32, (phenos, TILE), 1) + begin
        inside = (row >= low_row) & (row < high_row)
        grad = grad_ref[:, cut] - jnp.where(inside, product_with(window[:, part], ld_ref[cut, part]), 0.0)
        if not far:
            refs[0][:, cut] = grad
            continue
        refs[2][:, cut] = refs[1][:, cut] + grad
        resid = resid + chunk_sums(grad * grad)
    if far:
        spread(resid, refs[0][...], refs[3])


def align(along, firsts_ref, ld_ref, out_ref, wide):
    rows, span = ld_ref.shape
    place = lax.axis_index(along)
    base = place * rows
    left = lax.rem(place, 2) == 0
    gap = span + LANES
    table = firsts_ref[...]
    count = 2 * rows // LANES
    first = table[0, 0] - base
    last = table[0, count - 1] - base
    lane = lax.broadcasted_iota(jnp.int32, table.shape, 1)
    ends = jnp.where((lane < count) & (table - base != first), table - base, rows)
    end = jnp.min(ends.astype(jnp.float32), axis=1, keepdims=True).astype(jnp.int32)
    low_row = jnp.where(left, 0, last)
    high_row = jnp.where(left, end, rows)
    start = jnp.where(left, gap - first - span, gap + span - jnp.maximum(last, 0))
    wide[:, :gap] = jnp.zeros((TILE, gap), wide.dtype)
    wide[:, gap + span :] = jnp.zeros((TILE, gap), wide.dtype)

    tiles = rows // TILE
    for turn in range(tiles):
        width = span - turn * TILE
        begin = pl.multiple_of(jnp.where(left, turn, tiles - 1 - turn) * TILE, TILE)
        side = pl.multiple_of(jnp.where(left, span - width, 0), TILE)
        row = lax.broadcasted_iota(jnp.int32, (TILE, LANES), 0) + begin
        inside = (row >= low_row) & (row < high_row)
        wide[:, gap : gap + span] = ld_ref[pl.ds(begin, TILE)]

        def store(cut, values, begin=begin, side=side):
            out_ref[pl.ds(begin, TILE), pl.ds(pl.multiple_of(side + cut.start, LANES), LANES)] = values

        turned(wide, start + side, width, store, inside)


def finish(along, halo_ref, far_ld_ref, grad_ref, scale_ref, beta_ref, value_ref, out_ref):
    rows, span = far_ld_ref.shape
    phenos = halo_ref.shape[0]
    left = lax.rem(lax.axis_index(along), 2) == 0
    resid = jnp.zeros((phenos, LANES), jnp.float32)
    tiles = rows // TILE
    for turn in range(tiles):
        width = span - turn * TILE
        begin = pl.multiple_of(jnp.where(left, turn, tiles - 1 - turn) * TILE, TILE)
        cut, part = pl.ds(begin, TILE), pl.ds(pl.multiple_of(jnp.where(left, span - width, 0), TILE), width)
        grad = grad_ref[:, cut] - product_with(halo_ref[:, part], far_ld_ref[cut, part])
        value_ref[:, cut] = beta_ref[:, cut] + grad
        resid = resid + chunk_sums(grad * grad)
    spread(resid, scale_ref[...], out_ref)


def shards(ld_rows, block_first, beta_hat, psi, noise, sample_size):
    rows, span = ld_rows.shape
    phenos = beta_hat.shape[0]
    blocks, groups = lax.axis_size("blk"), lax.axis_size("phe")
    assert rows == span and rows % TILE == 0, rows
    snps = rows * blocks
    every = ("blk", "phe")
    vmem = pl.BlockSpec(memory_space=pltpu.VMEM)
    smem = pl.BlockSpec(memory_space=pltpu.SMEM)
    hbm = pl.BlockSpec(memory_space=pltpu.HBM)
    wide_shape = pltpu.VMEM(beta_hat.shape, jnp.float32)
    low_shape = pltpu.VMEM(beta_hat.shape, jnp.bfloat16)
    sums_shape = pltpu.VMEM((blocks * groups, 2 * phenos), jnp.float32)
    params = pltpu.CompilerParams(vmem_limit_bytes=16 << 20)

    def here(argument):
        return pltpu.with_memory_space_constraint(argument, pltpu.HBM)

    def total(sums):
        return lax.all_to_all(sums, every, 0, 0, tiled=True)

    beta_hat, psi, noise, sample_size, sums = pl.pallas_call(
        begin,
        in_specs=[hbm] * 4,
        out_specs=[vmem] * 5,
        out_shape=[
            wide_shape,
            wide_shape,
            pltpu.VMEM(noise.shape, noise.dtype),
            pltpu.VMEM((1, phenos), jnp.int32),
            sums_shape,
        ],
        scratch_shapes=[pltpu.SemaphoreType.DMA((4,))],
        compiler_params=params,
    )(*map(here, (beta_hat, psi, noise, sample_size[None])))
    sums = total(sums)

    def step(t, sums, value):
        last = t == ITERS - 1
        return pl.pallas_call(
            functools.partial(update, "phe", groups, snps, t),
            in_specs=[vmem] * 5,
            out_specs=vmem if last else [vmem] * 2,
            out_shape=jax.ShapeDtypeStruct(beta_hat.shape, jnp.float32) if last else [wide_shape, low_shape],
            compiler_params=params,
        )(sums, sample_size, value, psi, noise)

    far = [(i, i + 1 if i % 2 else i - 1) for i in range(1, blocks - 1 + blocks % 2)]
    near = [(i, i ^ 1) for i in range(blocks - blocks % 2)]
    value = beta_hat
    for t in range(ITERS - 1):
        beta, low = step(t, sums, value)
        far_low = lax.ppermute(low, "blk", far)
        near_low = lax.ppermute(low, "blk", near)
        if t == 0:
            ld_rows, firsts = pl.pallas_call(
                load,
                in_specs=[vmem] + [hbm] * 2,
                out_specs=[vmem] * 2,
                out_shape=[pltpu.VMEM(ld_rows.shape, ld_rows.dtype), pltpu.VMEM((1, LANES), jnp.int32)],
                scratch_shapes=[pltpu.VMEM((rows // LANES, LANES), jnp.int32), pltpu.SemaphoreType.DMA((2,))],
                compiler_params=params,
                cost_estimate=pl.CostEstimate(flops=1 << 26, bytes_accessed=3 << 20, transcendentals=0),
            )(low, here(block_first.reshape(-1, LANES)), here(ld_rows))
        grad, scale = pl.pallas_call(
            functools.partial(inner, "blk"),
            in_specs=[smem] + [vmem] * 5,
            out_specs=[vmem] * 2,
            out_shape=[wide_shape, pltpu.VMEM((phenos, LANES), jnp.float32)],
            scratch_shapes=[
                pltpu.VMEM((phenos, 3 * span + LANES), jnp.bfloat16),
                pltpu.VMEM((2 * rows // LANES + WINDOWS, phenos, span), jnp.bfloat16),
                pltpu.SMEM((2 * rows // LANES,), jnp.int32),
            ],
            compiler_params=params,
            cost_estimate=pl.CostEstimate(flops=2 * WINDOWS * phenos * rows * span, bytes_accessed=4 << 20, transcendentals=0),
        )(firsts, low, ld_rows, beta_hat, psi, beta)
        sides = [pltpu.VMEM((phenos, 3 * span + 2 * LANES), jnp.bfloat16), pltpu.VMEM((phenos, span), jnp.bfloat16)]
        grad = pl.pallas_call(
            functools.partial(outer, "blk", False),
            in_specs=[vmem] * 4,
            out_specs=vmem,
            out_shape=wide_shape,
            scratch_shapes=sides,
            compiler_params=params,
            cost_estimate=pl.CostEstimate(flops=2 * phenos * rows * span, bytes_accessed=3 << 20, transcendentals=0),
        )(firsts, near_low, ld_rows, grad)
        if t == 0:
            far_ld = pl.pallas_call(
                functools.partial(align, "blk"),
                in_specs=[vmem] * 2,
                out_specs=vmem,
                out_shape=pltpu.VMEM(ld_rows.shape, ld_rows.dtype),
                scratch_shapes=[pltpu.VMEM((TILE, 3 * span + 2 * LANES), jnp.bfloat16)],
                compiler_params=params,
                cost_estimate=pl.CostEstimate(flops=1 << 26, bytes_accessed=4 << 20, transcendentals=0),
            )(firsts, ld_rows)
        value, sums = pl.pallas_call(
            functools.partial(finish, "blk"),
            in_specs=[vmem] * 5,
            out_specs=[vmem] * 2,
            out_shape=[wide_shape, sums_shape],
            compiler_params=params,
        )(far_low, far_ld, grad, scale, beta)
        sums = total(sums)
    return step(ITERS - 1, sums, value)


def solution(mesh):
    in_specs = (
        P("blk", None),
        P("blk"),
        P("phe", "blk"),
        P("phe", "blk"),
        P(None, "phe", "blk"),
        P("phe"),
    )
    out_specs = P("phe", "blk")
    return jax.shard_map(shards, mesh=mesh, in_specs=in_specs, out_specs=out_specs, check_vma=False)
```
